32 devices in a mesh: row: 4 (over x, core), col: 4 (over z), depth: 2 (over y).
Axes of the slice: x: 2, y: 2, z: 4, core: 2. Of those that a mesh axis runs over, the one named last changes fastest.
Arguments:
- trailing: float32 [3008, 48128], P('depth', ('row', 'col')), may hold values from -6 to 6
- panel_block: float32 [48128, 1024], P(('row', 'col', 'depth')), may hold values from -6 to 6
- factor_panel: float32 [48128, 1024], P(('row', 'col', 'depth')), may hold values from -0.1875 to 0.1875
- corner_block: float32 [1024, 1024], P(('row', 'col', 'depth')), may hold values from -6 to 6, as said below
- corner_inverse: float32 [1024, 1024], P(('row', 'col', 'depth')), may hold values from -1 to 2, as said below
Outputs:
- trailing_out: float32 [3008, 48128], P('depth', ('row', 'col'))
- panel_out: float32 [48128, 1024], P(('row', 'col', 'depth'))
- corner_out: float32 [1024, 1024], P(('row', 'col', 'depth'))
The draws below stay inside these ranges and needn't reach their ends.
Inputs may be any that keep to these rules, and one draw needn't show every extreme that they name: `corner_block`: symmetric. `corner_inverse`: lower triangular, diagonal between 1 and 2.
All inputs are finite; a program needn't handle non-finite values.
Results may differ from the reference program's by a relative error of at most 0.00012.
Values sent between devices are 32-bit elements; how exact they have to be, the bound alone decides.
A program may use at most 192 MiB of HBM per device.

```python
import jax
import jax.numpy as jnp
from jax import lax

NB = 1024
M = 48128
SPAN = 1
SLAB = 3008
N_DEPTH = 2


def draw_corner_block(key, part):
    noise = jax.random.truncated_normal(jax.random.fold_in(key, 11), -4.0, 4.0, (NB, NB), jnp.float32)
    return (noise + noise.T) * 0.7071


def draw_corner_inverse(key, part):
    below = jax.random.truncated_normal(jax.random.fold_in(key, 23), -4.0, 4.0, (NB, NB), jnp.float32)
    diagonal = jax.random.uniform(jax.random.fold_in(key, 29), (NB,), jnp.float32, 1.0, 2.0)
    strict = jnp.tril(below, -1) * (0.5 / NB ** 0.5)
    return strict + jnp.diag(diagonal)


def block_scale(rng, shape, cuts, least, largest):
    level = 1.0
    for position, shards_of in cuts:
        draws = jax.random.uniform(jax.random.fold_in(jax.random.fold_in(rng, 6), position), (shards_of,), jnp.float32, least / len(cuts), largest / len(cuts))
        level = level * jnp.repeat(jnp.exp(draws), shape[position] // shards_of).reshape((-1,) + (1,) * (len(shape) - 1 - position))
    return level


def gaussian(stream_key, shape, scale, limit, cuts=(), dtype=jnp.bfloat16):
    loudness = block_scale(stream_key, shape, cuts, -0.22, 0.18) if cuts else 1.0
    array = jax.random.normal(stream_key, shape, jnp.float32) * scale * loudness
    return jnp.minimum(jnp.maximum(array, -limit), limit).astype(dtype)


def setup_inputs(seed: int = 0) -> dict:
    arg_keys = jax.random.split(jax.random.key(seed), 6)
    trailing = gaussian(arg_keys[0], (SLAB, M), 1.0, 6.0, ((0, 2), (1, 16)), jnp.float32)
    panel_block = gaussian(arg_keys[1], (M, NB), 1.0, 6.0, ((0, 32),), jnp.float32)
    factor_panel = gaussian(arg_keys[2], (M, NB), NB ** -0.5, 0.1875, ((0, 32),), jnp.float32)
    corner_block = draw_corner_block(jax.random.fold_in(arg_keys[5], 71), 0)
    corner_inverse = draw_corner_inverse(jax.random.fold_in(arg_keys[5], 71), 0)
    return dict(trailing=trailing, panel_block=panel_block, factor_panel=factor_panel, corner_block=corner_block, corner_inverse=corner_inverse)


def matmul(left, right):
    return jnp.dot(left, right, precision=lax.Precision.HIGHEST, preferred_element_type=jnp.float32)


def permute(matrix):
    block = matrix[:SLAB]
    shaped = block.reshape(SPAN, N_DEPTH, SLAB // (SPAN * N_DEPTH), block.shape[1])
    return jnp.transpose(shaped, (1, 0, 2, 3)).reshape(SLAB, block.shape[1])


def reference(trailing, panel_block, factor_panel, corner_block, corner_inverse):
    corner_out = matmul(corner_inverse, matmul(corner_block, corner_inverse.T))
    scaled = matmul(panel_block, corner_inverse.T)
    coupling = matmul(factor_panel, corner_out)
    half_panel = scaled - 0.5 * coupling
    panel_out = half_panel - 0.5 * coupling
    update = matmul(permute(half_panel), factor_panel.T) + matmul(permute(factor_panel), half_panel.T)
    trailing_out = trailing - update
    return trailing_out, panel_out, corner_out
```

```python
import functools

import jax
import jax.numpy as jnp
from jax import lax
from jax.experimental import pallas as pl
from jax.experimental.pallas import tpu as pltpu
from jax.sharding import PartitionSpec as P


EVERY = ("row", "col", "depth")
MESH = pl.DeviceIdType.MESH
TILE = 256
LIMIT = 60 * 1024 * 1024
ANY = pl.BlockSpec(memory_space=pl.ANY)


def matmul(left, right):
    return jnp.dot(left, right, precision=lax.Precision.HIGH, preferred_element_type=jnp.float32)


def contract(left, right):
    return lax.dot_general(
        left,
        right,
        (((1,), (1,)), ((), ())),
        precision=lax.Precision.HIGH,
        preferred_element_type=jnp.float32,
    )


def pack_corner(corner_block, corner_inverse):
    rows, width = corner_inverse.shape
    first = lax.axis_index(EVERY) * rows
    row = first + lax.broadcasted_iota(jnp.int32, (rows, width), 0)
    col = lax.broadcasted_iota(jnp.int32, (rows, width), 1)
    both = jnp.where(col > row, corner_block, corner_inverse)
    diagonal = jnp.sum(jnp.where(col == row, corner_block, 0.0), axis=1, keepdims=True)
    return jnp.concatenate([both, jnp.broadcast_to(diagonal, (rows, 128))], axis=1)


def unpack_corner(packed, width):
    row = lax.broadcasted_iota(jnp.int32, (width, width), 0)
    col = lax.broadcasted_iota(jnp.int32, (width, width), 1)
    both = packed[:, :width]
    inverse = jnp.where(col <= row, both, 0.0)
    upper = jnp.where(col > row, both, jnp.where(col == row, 0.5 * packed[:, width:width + 1], 0.0))
    return inverse, upper


def transform(panel, factor, inverse, corner):
    coupling = matmul(factor, corner)
    half = contract(panel, inverse) - 0.5 * coupling
    return half - 0.5 * coupling


def exchange(value, layers):
    blocks = [value]
    for shift in range(1, layers):
        pairs = [(source, (source + shift) % layers) for source in range(layers)]
        blocks.append(lax.ppermute(value, "depth", pairs))
    return blocks


def arrange(blocks, layers):
    if layers == 1:
        return blocks[0]
    me = lax.axis_index("depth")
    rows, width = blocks[0].shape
    whole = jnp.zeros((layers * rows, width), blocks[0].dtype)
    for shift, block in enumerate(blocks):
        place = lax.rem(me - shift + layers, layers)
        whole = lax.dynamic_update_slice(whole, block, (place * rows, 0))
    return whole


def make_general(layers):
    def body(trailing, panel_block, factor_panel, corner_block, corner_inverse):
        rows, width = panel_block.shape
        factor_blocks = exchange(factor_panel, layers)
        panel_blocks = exchange(panel_block, layers)
        packed = lax.all_gather(pack_corner(corner_block, corner_inverse), EVERY, axis=0, tiled=True)
        source = lax.axis_index(("row", "col")) == 0
        kept = jnp.where(source, jnp.concatenate((panel_block, factor_panel), axis=0), 0.0)
        slab = lax.psum(kept, ("row", "col"))
        inverse, upper = unpack_corner(packed, width)
        triangle = matmul(inverse, contract(upper, inverse))
        corner = triangle + triangle.T
        corner_rows = corner_inverse.shape[0]
        corner_out = lax.dynamic_slice(
            corner, (lax.axis_index(EVERY) * corner_rows, 0), (corner_rows, width)
        )
        panel_out = transform(panel_block, factor_panel, inverse, corner)
        factor_cols = arrange(factor_blocks, layers)
        panel_cols = arrange(panel_blocks, layers)
        left = transform(slab[:rows], slab[rows:], inverse, corner)
        right = matmul(slab[rows:], inverse)
        trailing_out = (trailing - contract(left, factor_cols)) - contract(right, panel_cols)
        return (trailing_out, panel_out, corner_out)

    return body


def after(value, earlier):
    return lax.optimization_barrier((value, earlier))[0]


def spread_kernel(ncol, piece, packed, panel, factor, corner, ps, fs,
                  yl, zr, zl, xr, cr, sz, sx, sc, rm, rp, su, sd, sq):
    r, c, d = lax.axis_index("row"), lax.axis_index("col"), lax.axis_index("depth")
    x, core = r // 2, r % 2
    across, mate = (1 - x) * 2 + core, x * 2 + (1 - core)
    block = packed.shape[0]
    count = ps.shape[0] // piece
    source = (r == 0) & (c == 0)

    def at(ref, first, size):
        return ref.at[pl.ds(pl.multiple_of(first, 8), size)]

    def remote(src, dst, send, recv, row, col, depth):
        return pltpu.make_async_remote_copy(
            src_ref=src, dst_ref=dst, send_sem=send, recv_sem=recv,
            device_id=(row, col, depth), device_id_type=MESH)

    keep = pltpu.make_async_copy(packed, at(corner, (r * ncol + c) * block, block), yl)
    keep.start()

    def each(body):
        def step(k, carry):
            body(k, pl.ds(pl.multiple_of(k * piece, 8), piece))
            return carry

        lax.fori_loop(0, count, step, 0)

    keep.wait()

    def rows_of(row, col):
        return at(corner, (row * ncol + col) * block, block)

    def forward_line(col, right, left):
        b = rows_of(r, col)

        if right:
            @pl.when(c < ncol - 1)
            def _():
                remote(b, b, sz.at[0, col], zr.at[col], r, c + 1, d).start()
        if left:
            @pl.when(c > 0)
            def _():
                remote(b, b, sz.at[1, col], zl.at[col], r, c - 1, d).start()
        remote(b, b, sx.at[col], xr.at[col], across, c, d).start()
        remote(b, b, sc.at[0, col], cr.at[0, col], mate, c, d).start()

    forward_line(c, True, True)

    @pl.when(source)
    def _():
        def body(k, s):
            remote(factor.at[s], fs.at[s], su, rm.at[k], 0, 1, d).start()
            remote(panel.at[s], ps.at[s], sd, rm.at[k], 3, 0, d).start()
            remote(factor.at[s], fs.at[s], sq.at[0], rp, 1, 0, d).start()
            remote(panel.at[s], ps.at[s], sq.at[1], rm.at[k], 1, 0, d).start()

        each(body)

    for s in range(1, ncol):
        @pl.when(c - s >= 0)
        def _():
            b = rows_of(r, c - s)
            remote(b, b, sz.at[0, c - s], zr.at[c - s], r, c, d).wait_recv()
            forward_line(c - s, True, False)

        @pl.when(c + s < ncol)
        def _():
            b = rows_of(r, c + s)
            remote(b, b, sz.at[1, c + s], zl.at[c + s], r, c, d).wait_recv()
            forward_line(c + s, False, True)

    def across_block(col):
        b = rows_of(across, col)
        remote(b, b, sx.at[col], xr.at[col], across, c, d).wait_recv()
        remote(b, b, sc.at[1, col], cr.at[1, col], mate, c, d).start()

    across_block(c)
    for s in range(1, ncol):
        @pl.when(c - s >= 0)
        def _():
            across_block(c - s)

        @pl.when(c + s < ncol)
        def _():
            across_block(c + s)

    trunk = x == core

    def stream(ref, other, own):
        up = trunk & (c < ncol - 1) & jnp.logical_not(source)
        side = trunk & (c > 0)
        down = (own == 0) & (x == 1) & (c == 1)
        local = (x > 0) | (c > 0)

        @pl.when(jnp.logical_not(source))
        def _():
            def body(k, s):
                v = ref.at[s]
                remote(v, v, su, rm.at[k], r, c, d).wait_recv()

                @pl.when(up)
                def _():
                    remote(v, v, su, rm.at[k], r, c + 1, d).start()

                @pl.when(side)
                def _():
                    remote(v, v, sd, rm.at[k], across, c, d).start()

                @pl.when(down)
                def _():
                    remote(v, v, sd, rm.at[k], r, 0, d).start()

                @pl.when(local)
                def _():
                    remote(v, v, sq.at[0], rp, mate, c, d).start()

            each(body)
            remote(other, other, su, rp, r, c, d).wait_recv()

            @pl.when(up)
            def _():
                remote(ref, ref, su, rp, r, c, d).wait_send()

            @pl.when(side | down)
            def _():
                remote(ref, ref, sd, rp, r, c, d).wait_send()

            @pl.when(local)
            def _():
                remote(ref, ref, sq.at[0], rp, r, c, d).wait_send()

    @pl.when(core == 0)
    def _():
        stream(fs, ps, 0)

    @pl.when(core == 1)
    def _():
        stream(ps, fs, 1)

    @pl.when(source)
    def _():
        for sem in (su, sd, sq.at[0], sq.at[1]):
            remote(ps, ps, sem, rp, r, c, d).wait_send()

    for col in range(ncol):
        for half in range(2):
            b = rows_of(0, col)
            remote(b, b, sc.at[half, col], cr.at[half, col], mate, c, d).wait()
        remote(b, b, sx.at[col], rp, r, c, d).wait_send()

        @pl.when((c < ncol - 1) & (col <= c))
        def _():
            b = rows_of(0, col)
            remote(b, b, sz.at[0, col], rp, r, c, d).wait_send()

        @pl.when((c > 0) & (col >= c))
        def _():
            b = rows_of(0, col)
            remote(b, b, sz.at[1, col], rp, r, c, d).wait_send()


def spread(packed, panel, factor, ncol, devices):
    rows = panel.shape[0]
    piece = 32
    count = rows // piece
    dma = pltpu.SemaphoreType.DMA
    return pl.pallas_call(
        functools.partial(spread_kernel, ncol, piece),
        out_shape=(
            jax.ShapeDtypeStruct((packed.shape[0] * devices // 2, packed.shape[1]), jnp.float32),
            jax.ShapeDtypeStruct(panel.shape, jnp.float32),
            jax.ShapeDtypeStruct(panel.shape, jnp.float32),
        ),
        in_specs=[ANY] * 3,
        out_specs=(ANY,) * 3,
        scratch_shapes=[
            dma, dma((ncol,)), dma((ncol,)), dma((ncol,)), dma((2, ncol)),
            dma((2, ncol)), dma((ncol,)), dma((2, ncol)),
            dma((count,)), dma, dma, dma, dma((2,)),
        ],
        compiler_params=pltpu.CompilerParams(has_side_effects=True, vmem_limit_bytes=8 * 1024 * 1024),
        cost_estimate=pl.CostEstimate(flops=100_000_000, bytes_accessed=40_000_000, transcendentals=0),
        name="spread",
    )(packed, panel, factor)


def halves(value):
    high = value.astype(jnp.bfloat16)
    low = (value - high.astype(jnp.float32)).astype(jnp.bfloat16)
    return high, low


def dot(left, right, transposed):
    dims = (((1,), (1 if transposed else 0,)), ((), ()))
    return lax.dot_general(left, right, dims, preferred_element_type=jnp.float32)


def dot3(left, right, transposed):
    high, low = left
    return dot(high, right[0], transposed) + (dot(high, right[1], transposed) + dot(low, right[0], transposed))


def unpack_kernel(size, wide, tall, ih, il, ah, al):
    i = pl.program_id(0)
    width = ih.shape[1]
    both = wide[:, :width]
    row = i * size + lax.broadcasted_iota(jnp.int32, (size, width), 0)
    col = lax.broadcasted_iota(jnp.int32, (size, width), 1)
    ih[...], il[...] = halves(jnp.where(col <= row, both, 0.0))
    below = tall[...].T
    diagonal = wide[:, width:width + 1]
    ah[...], al[...] = halves(jnp.where(col > row, both, jnp.where(col == row, diagonal, below)))


def unpack(packed):
    width = packed.shape[0]
    size = 128
    out = jax.ShapeDtypeStruct((width, width), jnp.bfloat16)
    return pl.pallas_call(
        functools.partial(unpack_kernel, size),
        grid=(width // size,),
        out_shape=(out,) * 4,
        in_specs=[
            pl.BlockSpec((size, packed.shape[1]), lambda i: (i, 0)),
            pl.BlockSpec((width, size), lambda i: (0, i)),
        ],
        out_specs=(pl.BlockSpec((size, width), lambda i: (i, 0)),) * 4,
        compiler_params=pltpu.CompilerParams(vmem_limit_bytes=LIMIT),
        cost_estimate=pl.CostEstimate(flops=100_000_000, bytes_accessed=17_000_000, transcendentals=0),
        name="unpack",
    )(packed, packed)


def split_kernel(source, a, b, ours, theirs, ah, al, bh, bl):
    mine = source[0] == 1
    ah[...], al[...] = halves(jnp.where(mine, ours[...], a[...]))
    bh[...], bl[...] = halves(jnp.where(mine, theirs[...], b[...]))


def split(a, b, ours, theirs, source):
    rows, width = a.shape
    spec = pl.BlockSpec((128, width), lambda i, s: (i, 0))
    came = pl.BlockSpec((128, width), lambda i, s: (i * (1 - s[0]), 0))
    kept = pl.BlockSpec((128, width), lambda i, s: (i * s[0], 0))
    out = jax.ShapeDtypeStruct((rows, width), jnp.bfloat16)
    return pl.pallas_call(
        split_kernel,
        grid_spec=pltpu.PrefetchScalarGridSpec(
            num_scalar_prefetch=1,
            grid=(pl.cdiv(rows, 128),),
            in_specs=[came] * 2 + [kept] * 2,
            out_specs=(spec,) * 4,
        ),
        out_shape=(out,) * 4,
        compiler_params=pltpu.CompilerParams(vmem_limit_bytes=LIMIT),
        cost_estimate=pl.CostEstimate(flops=100_000_000, bytes_accessed=25_000_000, transcendentals=0),
        name="split",
    )(source, a, b, ours, theirs)


def columns_kernel(rows, unit, first, factor, panel, ih, il, ah, al, g, q, *corner):
    i = pl.program_id(0)
    f, p = factor[...], panel[...]
    if unit:
        row = i * TILE + lax.broadcasted_iota(jnp.int32, f.shape, 0)
        col = lax.broadcasted_iota(jnp.int32, f.shape, 1)
        f = jnp.where(row < rows, f, jnp.where(col == first[0] + row - rows, -1.0, 0.0))
        p = jnp.where(row < rows, p, 0.0)
    inverse = (ih[...], il[...])
    gg = dot3(halves(f), inverse, False)
    g[...] = gg
    z = p - dot3(halves(gg), (ah[...], al[...]), False)
    qq = dot3(halves(z), inverse, True)
    q[...] = qq
    if unit:
        corner[0][...] = qq[rows % TILE:rows % TILE + unit]


def columns(factor, panel, weights, unit=0):
    rows, width = factor.shape
    spec = pl.BlockSpec((TILE, width), lambda i, s: (i, 0))
    fixed = pl.BlockSpec((width, width), lambda i, s: (0, 0))
    out = jax.ShapeDtypeStruct((rows, width), jnp.float32)
    shapes, specs = [out, out], [spec, spec]
    if unit:
        shapes.append(jax.ShapeDtypeStruct((unit, width), jnp.float32))
        specs.append(pl.BlockSpec((unit, width), lambda i, s: (0, 0)))
    first = jnp.reshape(lax.axis_index(EVERY) * unit, (1,)).astype(jnp.int32)
    return pl.pallas_call(
        functools.partial(columns_kernel, rows, unit),
        grid_spec=pltpu.PrefetchScalarGridSpec(
            num_scalar_prefetch=1,
            grid=(pl.cdiv(rows, TILE),),
            in_specs=[spec, spec] + [fixed] * 4,
            out_specs=tuple(specs),
        ),
        out_shape=tuple(shapes),
        compiler_params=pltpu.CompilerParams(vmem_limit_bytes=LIMIT),
        cost_estimate=pl.CostEstimate(flops=18 * rows * width * width, bytes_accessed=16 * rows * width, transcendentals=0),
        name="columns",
    )(first, factor, panel, *weights)


def update_kernel(tiles, ph, plo, fh, fl, g, q, trailing, *refs):
    out = refs[-1]
    rows = ph.shape[0]
    step = 512
    gg, qq = halves(g[...]), halves(q[...])
    starts = [min(k * step, rows - step) for k in range(pl.cdiv(rows, step))]
    for s in starts:
        part = slice(s, s + step)
        u = dot3((ph[part], plo[part]), gg, True) + dot3((fh[part], fl[part]), qq, True)
        out[part] = trailing[part] - u


def update(trailing, slab, g, q, tiles, out, offset=None):
    rows, width = slab[0].shape
    fixed = pl.BlockSpec((rows, width), lambda i, t: (0, 0), pipeline_mode=pl.Buffered(1))
    tall = pl.BlockSpec((rows, TILE), lambda i, t: (0, t[i]))
    wide = pl.BlockSpec((TILE, width), lambda i, t: (i, 0))
    count = tiles.shape[0]
    if offset is not None:
        over = TILE - rows % TILE + TILE
        wide = pl.BlockSpec(
            (pl.Element(TILE, padding=(0, over)), pl.Element(width)),
            lambda i, t: (pl.multiple_of(i * TILE + t[count], 8), 0))
        tiles = jnp.concatenate([tiles, jnp.reshape(offset, (1,)).astype(jnp.int32)])
    args = [tiles, *slab, g, q, trailing]
    specs = [fixed] * 4 + [wide, wide, tall]
    alias = {}
    if out is not None:
        alias = {len(args): 0}
        args.append(out)
        specs.append(ANY)
    return pl.pallas_call(
        update_kernel,
        grid_spec=pltpu.PrefetchScalarGridSpec(
            num_scalar_prefetch=1, grid=(count,), in_specs=specs, out_specs=tall),
        out_shape=jax.ShapeDtypeStruct(trailing.shape, jnp.float32),
        input_output_aliases=alias,
        compiler_params=pltpu.CompilerParams(vmem_limit_bytes=LIMIT),
        cost_estimate=pl.CostEstimate(flops=12 * rows * width * TILE * count, bytes_accessed=12 * rows * TILE * count, transcendentals=0),
        name="update",
    )(*args)


def make_fast(ncol, devices):
    swap = [(0, 1), (1, 0)]

    def body(trailing, panel_block, factor_panel, corner_block, corner_inverse):
        rows, width = panel_block.shape
        d = lax.axis_index("depth")
        low = rows // TILE
        shift = (low + 1) * TILE - rows
        rest = rows - low * TILE

        def cut(value, first, size):
            return lax.dynamic_slice(value, (first + shift * d, 0), (size, width))

        def send(value):
            return lax.ppermute(value, "depth", swap)

        early = low - 1
        packed = pack_corner(corner_block, corner_inverse)
        theirs = send(packed)
        pair = jnp.where(d == 1, jnp.concatenate([theirs, packed], axis=0), jnp.concatenate([packed, theirs], axis=0))
        factor_first, panel_first = after((factor_panel, panel_block), pair)
        sizes = [early * TILE]
        firsts = [0]
        raw = []
        for f, s in zip(firsts, sizes):
            fc = send(cut(factor_first, f, s))
            pc = send(cut(panel_first, f, s))
            raw.append((fc, pc))

        packed, ps, fs = spread(pair, panel_first, factor_first, ncol, devices)
        weights = unpack(packed)
        source = (lax.axis_index(("row", "col")) == 0).astype(jnp.int32)
        slab = split(ps, fs, panel_block, factor_panel, jnp.reshape(source, (1,)))
        g, panel_out, corner_out = columns(factor_panel, panel_block, weights, corner_inverse.shape[0])

        done = []
        if low > early:
            done.append((early * TILE, (send(cut(g, early * TILE, TILE)), send(cut(panel_out, early * TILE, TILE)))))

        def last(value):
            high = jnp.concatenate([value[low * TILE + shift:], value[:shift]], axis=0)
            return jnp.where(d == 1, high, value[low * TILE:])

        def ids(first, count):
            return (first + jnp.arange(count)).astype(jnp.int32)

        base = d * (low + 1)
        other = (1 - d) * (low + 1)
        out = update(trailing, slab, g, panel_out, ids(base, pl.cdiv(rows - shift, TILE)), None, shift * d)
        tail = after((last(g), last(panel_out)), out)
        tail = (send(tail[0]), send(tail[1]))
        for f, s, pair in zip(firsts, sizes, raw):
            gc, qc = columns(*after(pair, out), weights)
            out = update(trailing, slab, gc, qc, ids(other + f // TILE, s // TILE), out)
        for f, pair in done:
            gc, qc = after(pair, out)
            out = update(trailing, slab, gc, qc, ids(other + f // TILE, 1), out)

        def final(value, mine):
            head = value[:rest - shift]
            end = value[rest - shift:]
            first = jnp.concatenate([head, end, mine[:shift]], axis=0)
            second = jnp.concatenate([mine[low * TILE:], end], axis=0)
            return jnp.concatenate([first, jnp.where(d == 1, first, second)], axis=0)

        tail = after(tail, out)
        last_ids = jnp.stack([jnp.where(d == 1, low, other + low), low]).astype(jnp.int32)
        out = update(trailing, slab, final(tail[0], g), final(tail[1], panel_out), last_ids, out)
        return (out, panel_out, corner_out)

    return body


def solution(mesh):
    in_specs = (
        P("depth", ("row", "col")),
        P(EVERY, None),
        P(EVERY, None),
        P(EVERY, None),
        P(EVERY, None),
    )
    out_specs = (
        P("depth", ("row", "col")),
        P(EVERY, None),
        P(EVERY, None),
    )
    layers, nrow, ncol = mesh.shape["depth"], mesh.shape["row"], mesh.shape["col"]
    general = make_general(layers)

    def body(*args):
        rows = args[1].shape[0]
        unit = args[4].shape[0]
        fits = layers == 2 and nrow == 4 and ncol > 1 and rows % 32 == 0 and rows > 2 * TILE
        fits = fits and rows % TILE + unit == TILE and unit % 8 == 0
        chosen = make_fast(ncol, layers * nrow * ncol) if fits else general
        return chosen(*args)

    return jax.shard_map(body, mesh=mesh, in_specs=in_specs, out_specs=out_specs, check_vma=False)
```

```python
import functools

import jax
import jax.numpy as jnp
from jax import lax
from jax.experimental import pallas as pl
from jax.experimental.pallas import tpu as pltpu
from jax.sharding import PartitionSpec as P


EVERY = ("row", "col", "depth")
MESH = pl.DeviceIdType.MESH
TILE = 256
LIMIT = 60 * 1024 * 1024
ANY = pl.BlockSpec(memory_space=pl.ANY)


def matmul(left, right):
    return jnp.dot(left, right, precision=lax.Precision.HIGH, preferred_element_type=jnp.float32)


def contract(left, right):
    return lax.dot_general(
        left,
        right,
        (((1,), (1,)), ((), ())),
        precision=lax.Precision.HIGH,
        preferred_element_type=jnp.float32,
    )


def pack_corner(corner_block, corner_inverse):
    rows, width = corner_inverse.shape
    first = lax.axis_index(EVERY) * rows
    row = first + lax.broadcasted_iota(jnp.int32, (rows, width), 0)
    col = lax.broadcasted_iota(jnp.int32, (rows, width), 1)
    both = jnp.where(col > row, corner_block, corner_inverse)
    diagonal = jnp.sum(jnp.where(col == row, corner_block, 0.0), axis=1, keepdims=True)
    return jnp.concatenate([both, jnp.broadcast_to(diagonal, (rows, 128))], axis=1)


def unpack_corner(packed, width):
    row = lax.broadcasted_iota(jnp.int32, (width, width), 0)
    col = lax.broadcasted_iota(jnp.int32, (width, width), 1)
    both = packed[:, :width]
    inverse = jnp.where(col <= row, both, 0.0)
    upper = jnp.where(col > row, both, jnp.where(col == row, 0.5 * packed[:, width:width + 1], 0.0))
    return inverse, upper


def transform(panel, factor, inverse, corner):
    coupling = matmul(factor, corner)
    half = contract(panel, inverse) - 0.5 * coupling
    return half - 0.5 * coupling


def exchange(value, layers):
    blocks = [value]
    for shift in range(1, layers):
        pairs = [(source, (source + shift) % layers) for source in range(layers)]
        blocks.append(lax.ppermute(value, "depth", pairs))
    return blocks


def arrange(blocks, layers):
    if layers == 1:
        return blocks[0]
    me = lax.axis_index("depth")
    rows, width = blocks[0].shape
    whole = jnp.zeros((layers * rows, width), blocks[0].dtype)
    for shift, block in enumerate(blocks):
        place = lax.rem(me - shift + layers, layers)
        whole = lax.dynamic_update_slice(whole, block, (place * rows, 0))
    return whole


def make_general(layers):
    def body(trailing, panel_block, factor_panel, corner_block, corner_inverse):
        rows, width = panel_block.shape
        factor_blocks = exchange(factor_panel, layers)
        panel_blocks = exchange(panel_block, layers)
        packed = lax.all_gather(pack_corner(corner_block, corner_inverse), EVERY, axis=0, tiled=True)
        source = lax.axis_index(("row", "col")) == 0
        kept = jnp.where(source, jnp.concatenate((panel_block, factor_panel), axis=0), 0.0)
        slab = lax.psum(kept, ("row", "col"))
        inverse, upper = unpack_corner(packed, width)
        triangle = matmul(inverse, contract(upper, inverse))
        corner = triangle + triangle.T
        corner_rows = corner_inverse.shape[0]
        corner_out = lax.dynamic_slice(
            corner, (lax.axis_index(EVERY) * corner_rows, 0), (corner_rows, width)
        )
        panel_out = transform(panel_block, factor_panel, inverse, corner)
        factor_cols = arrange(factor_blocks, layers)
        panel_cols = arrange(panel_blocks, layers)
        left = transform(slab[:rows], slab[rows:], inverse, corner)
        right = matmul(slab[rows:], inverse)
        trailing_out = (trailing - contract(left, factor_cols)) - contract(right, panel_cols)
        return (trailing_out, panel_out, corner_out)

    return body


def after(value, earlier):
    return lax.optimization_barrier((value, earlier))[0]


def halves(value):
    high = value.astype(jnp.bfloat16)
    low = (value - high.astype(jnp.float32)).astype(jnp.bfloat16)
    return high, low


def dot(left, right, transposed):
    dims = (((1,), (1 if transposed else 0,)), ((), ()))
    return lax.dot_general(left, right, dims, preferred_element_type=jnp.float32)


def dot3(left, right, transposed):
    high, low = left
    return dot(high, right[0], transposed) + (dot(high, right[1], transposed) + dot(low, right[0], transposed))


def column_tile(f, p, ih, il, ah, al):
    width = f.shape[1]
    fh, fl = halves(f)
    gs = []
    for j in range(0, width, TILE):
        w = (ih[j:, j:j + TILE], il[j:, j:j + TILE])
        gs.append(dot3((fh[:, j:], fl[:, j:]), w, False))
    g = jnp.concatenate(gs, axis=1)
    z = p - dot3(halves(g), (ah[...], al[...]), False)
    zh, zl = halves(z)
    qs = []
    for j in range(TILE, width + TILE, TILE):
        w = (ih[j - TILE:j, :j], il[j - TILE:j, :j])
        qs.append(dot3((zh[:, :j], zl[:, :j]), w, True))
    return g, jnp.concatenate(qs, axis=1)


def spread_kernel(ncol, piece, packed, panel, factor,
                  ps, fs, ih_out, il_out, ah_out, al_out, g_out, q_out, corner_out, *more):
    (gs2, gs3, gtop, gend, qs2, qs3, qtop, qend,
     corner, ih, il, ah, al, fbuf, pbuf, gbuf, qbuf,
     yl, zr, zl, xr, cr, sz, sx, sc, rm, rp, su, sd, sq, loads, saves) = more
    r, c, d = lax.axis_index("row"), lax.axis_index("col"), lax.axis_index("depth")
    x, core = r // 2, r % 2
    across, mate = (1 - x) * 2 + core, x * 2 + (1 - core)
    block = packed.shape[0]
    rows, width = ps.shape
    count = rows // piece
    source = (r == 0) & (c == 0)

    def at(ref, first, size):
        return ref.at[pl.ds(pl.multiple_of(first, 8), size)]

    def remote(src, dst, send, recv, row, col, depth):
        return pltpu.make_async_remote_copy(
            src_ref=src, dst_ref=dst, send_sem=send, recv_sem=recv,
            device_id=(row, col, depth), device_id_type=MESH)

    keep = pltpu.make_async_copy(packed, at(corner, (r * ncol + c) * block, block), yl)
    keep.start()
    keep.wait()

    def rows_of(row, col):
        return at(corner, (row * ncol + col) * block, block)

    def forward_line(col, right, left):
        b = rows_of(r, col)

        if right:
            @pl.when(c < ncol - 1)
            def _():
                remote(b, b, sz.at[0, col], zr.at[col], r, c + 1, d).start()
        if left:
            @pl.when(c > 0)
            def _():
                remote(b, b, sz.at[1, col], zl.at[col], r, c - 1, d).start()
        remote(b, b, sx.at[col], xr.at[col], across, c, d).start()
        remote(b, b, sc.at[0, col], cr.at[0, col], mate, c, d).start()

    forward_line(c, True, True)

    load_f = pltpu.make_async_copy(factor, fbuf.at[:rows], loads.at[0])
    load_p = pltpu.make_async_copy(panel, pbuf.at[:rows], loads.at[1])
    load_f.start()
    load_p.start()

    trunk = x == core
    notsource = jnp.logical_not(source)
    up = trunk & (c < ncol - 1) & notsource
    side = trunk & (c > 0)
    down = (core == 0) & (x == 1) & (c == 1)
    local = (x > 0) | (c > 0)
    near = c == 0
    hops = jnp.where(core == 0, jnp.where(x == 0, c, jnp.where(near, 3, c + 1)),
                     jnp.where(x == 1, c + 1, jnp.where(near, 1, c + 2)))
    group = 3

    def pass_on(ref, j):
        def step(n, carry):
            k = j * group + n

            @pl.when(k < count)
            def _():
                v = ref.at[pl.ds(pl.multiple_of(k * piece, 8), piece)]
                remote(v, v, su, rm.at[k], r, c, d).wait_recv()

                @pl.when(up)
                def _():
                    remote(v, v, su, rm.at[k], r, c + 1, d).start()

                @pl.when(side)
                def _():
                    remote(v, v, sd, rm.at[k], across, c, d).start()

                @pl.when(down)
                def _():
                    remote(v, v, sd, rm.at[k], r, 0, d).start()

                @pl.when(local)
                def _():
                    remote(v, v, sq.at[0], rp, mate, c, d).start()

            return carry

        lax.fori_loop(0, group, step, 0)

    def begin(j):
        def step(n, carry):
            k = j * group + n

            @pl.when(k < count)
            def _():
                s = pl.ds(pl.multiple_of(k * piece, 8), piece)
                remote(factor.at[s], fs.at[s], su, rm.at[k], 0, 1, d).start()
                remote(panel.at[s], ps.at[s], sd, rm.at[k], 3, 0, d).start()
                remote(factor.at[s], fs.at[s], sq.at[0], rp, 1, 0, d).start()
                remote(panel.at[s], ps.at[s], sq.at[1], rm.at[k], 1, 0, d).start()

            return carry

        lax.fori_loop(0, group, step, 0)

    def position(i):
        @pl.when(source & (i * group < count))
        def _():
            begin(i)

        j = i - hops
        due = notsource & (j >= 0) & (j * group < count)

        @pl.when(due & (core == 0))
        def _():
            pass_on(fs, j)

        @pl.when(due & (core == 1))
        def _():
            pass_on(ps, j)

    done = 0
    position(done)
    for s in range(1, ncol):
        @pl.when(c - s >= 0)
        def _():
            b = rows_of(r, c - s)
            remote(b, b, sz.at[0, c - s], zr.at[c - s], r, c, d).wait_recv()
            forward_line(c - s, True, False)

        @pl.when(c + s < ncol)
        def _():
            b = rows_of(r, c + s)
            remote(b, b, sz.at[1, c + s], zl.at[c + s], r, c, d).wait_recv()
            forward_line(c + s, False, True)

        done += 1
        position(done)

    def across_block(col):
        b = rows_of(across, col)
        remote(b, b, sx.at[col], xr.at[col], across, c, d).wait_recv()
        remote(b, b, sc.at[1, col], cr.at[1, col], mate, c, d).start()

    across_block(c)
    done += 1
    position(done)
    for s in range(1, ncol):
        @pl.when(c - s >= 0)
        def _():
            across_block(c - s)

        @pl.when(c + s < ncol)
        def _():
            across_block(c + s)

        done += 1
        position(done)

    for col in range(ncol):
        for half in range(2):
            b = rows_of(0, col)
            remote(b, b, sc.at[half, col], cr.at[half, col], mate, c, d).wait()
        remote(b, b, sx.at[col], rp, r, c, d).wait_send()

        @pl.when((c < ncol - 1) & (col <= c))
        def _():
            b = rows_of(0, col)
            remote(b, b, sz.at[0, col], rp, r, c, d).wait_send()

        @pl.when((c > 0) & (col >= c))
        def _():
            b = rows_of(0, col)
            remote(b, b, sz.at[1, col], rp, r, c, d).wait_send()

    size = 128

    def unpack_step(i, carry):
        part = pl.ds(pl.multiple_of(i * size, size), size)
        wide = corner[part, :]
        both = wide[:, :width]
        row = i * size + lax.broadcasted_iota(jnp.int32, (size, width), 0)
        col = lax.broadcasted_iota(jnp.int32, (size, width), 1)
        ih[part, :], il[part, :] = halves(jnp.where(col <= row, both, 0.0))
        below = corner[:, part].T
        diagonal = wide[:, width:width + 1]
        ah[part, :], al[part, :] = halves(jnp.where(col > row, both, jnp.where(col == row, diagonal, below)))

        @pl.when(i % 2 == 1)
        def _():
            position(done + 1 + i // 2)

        return carry

    lax.fori_loop(0, width // size, unpack_step, 0)
    done += width // size // 2

    load_f.wait()
    load_p.wait()
    unit = fbuf.shape[0] - rows
    fbuf[rows:] = jnp.zeros((unit, width), jnp.float32)
    pbuf[rows:] = jnp.zeros((unit, width), jnp.float32)
    first = ((r * ncol + c) * 2 + d) * unit
    tiles = fbuf.shape[0] // TILE

    def columns_step(i, carry):
        part = pl.ds(pl.multiple_of(i * TILE, TILE), TILE)
        row = i * TILE + lax.broadcasted_iota(jnp.int32, (TILE, width), 0)
        col = lax.broadcasted_iota(jnp.int32, (TILE, width), 1)
        f = jnp.where(row < rows, fbuf[part, :], jnp.where(col == first + row - rows, -1.0, 0.0))
        gbuf[part, :], qbuf[part, :] = column_tile(f, pbuf[part, :], ih, il, ah, al)
        position(done + 1 + i)
        return carry

    lax.fori_loop(0, tiles, columns_step, 0)
    done += tiles

    outs = [
        pltpu.make_async_copy(gbuf.at[:rows], g_out, saves.at[0]),
        pltpu.make_async_copy(qbuf.at[:rows], q_out, saves.at[1]),
        pltpu.make_async_copy(qbuf.at[rows:], corner_out, saves.at[2]),
        pltpu.make_async_copy(ih, ih_out, saves.at[3]),
        pltpu.make_async_copy(il, il_out, saves.at[4]),
        pltpu.make_async_copy(ah, ah_out, saves.at[5]),
        pltpu.make_async_copy(al, al_out, saves.at[6]),
    ]
    low = rows // TILE
    cut = rows - gs3.shape[0] - gs2.shape[0]
    for buf, outs4 in ((gbuf, (gs2, gs3, gtop, gend)), (qbuf, (qs2, qs3, qtop, qend))):
        firsts = (cut, cut + gs2.shape[0], 0, low * TILE)
        for start, out in zip(firsts, outs4):
            outs.append(pltpu.make_async_copy(buf.at[start:start + out.shape[0]], out, saves.at[len(outs)]))
    for copy in outs:
        copy.start()

    last = pl.cdiv(count, group) + ncol + 1

    def rest(i, carry):
        position(i)
        return carry

    lax.fori_loop(done + 1, max(last, done + 1), rest, 0)

    @pl.when(notsource)
    def _():
        remote(ps, ps, su, rp, r, c, d).wait_recv()

        @pl.when(up)
        def _():
            remote(ps, ps, su, rp, r, c, d).wait_send()

        @pl.when(side | down)
        def _():
            remote(ps, ps, sd, rp, r, c, d).wait_send()

        @pl.when(local)
        def _():
            remote(ps, ps, sq.at[0], rp, r, c, d).wait_send()

    @pl.when(source)
    def _():
        for sem in (su, sd, sq.at[0], sq.at[1]):
            remote(ps, ps, sem, rp, r, c, d).wait_send()

    for copy in outs:
        copy.wait()


def spread(packed, panel, factor, unit, sizes, ncol, devices):
    rows, width = panel.shape
    piece = 32
    count = rows // piece
    dma = pltpu.SemaphoreType.DMA
    hbm = pl.BlockSpec(memory_space=pltpu.HBM)
    weight = (width, width)
    tall = (rows + unit, width)
    return pl.pallas_call(
        functools.partial(spread_kernel, ncol, piece),
        out_shape=tuple(
            [jax.ShapeDtypeStruct(panel.shape, jnp.float32)] * 2
            + [jax.ShapeDtypeStruct(weight, jnp.bfloat16)] * 4
            + [jax.ShapeDtypeStruct(panel.shape, jnp.float32)] * 2
            + [jax.ShapeDtypeStruct((n, width), jnp.float32) for n in (unit,) + sizes * 2]
        ),
        in_specs=[hbm] * 3,
        out_specs=(hbm,) * 17,
        scratch_shapes=[
            pltpu.VMEM((packed.shape[0] * devices // 2, packed.shape[1]), jnp.float32),
            *[pltpu.VMEM(weight, jnp.bfloat16)] * 4,
            *[pltpu.VMEM(tall, jnp.float32)] * 4,
            dma, dma((ncol,)), dma((ncol,)), dma((ncol,)), dma((2, ncol)),
            dma((2, ncol)), dma((ncol,)), dma((2, ncol)),
            dma((count,)), dma, dma, dma, dma((2,)), dma((2,)), dma((15,)),
        ],
        compiler_params=pltpu.CompilerParams(has_side_effects=True, vmem_limit_bytes=LIMIT),
        cost_estimate=pl.CostEstimate(flops=18 * rows * width * width, bytes_accessed=40_000_000, transcendentals=0),
        name="spread",
    )(packed, panel, factor)


def split_kernel(source, a, b, ours, theirs, q, out, kept):
    kept[...] = q[...]
    mine = source[0] == 1
    width = a.shape[1]
    out[:, width:2 * width], out[:, :width] = halves(jnp.where(mine, ours[...], a[...]))
    out[:, 2 * width:3 * width], out[:, 3 * width:] = halves(jnp.where(mine, theirs[...], b[...]))


def split(a, b, ours, theirs, q, source):
    rows, width = a.shape
    came = pl.BlockSpec((TILE, width), lambda i, s: (i * (1 - s[0]), 0))
    kept = pl.BlockSpec((TILE, width), lambda i, s: (i * s[0], 0))
    return pl.pallas_call(
        split_kernel,
        grid_spec=pltpu.PrefetchScalarGridSpec(
            num_scalar_prefetch=1,
            grid=(pl.cdiv(rows, TILE),),
            in_specs=[came] * 2 + [kept] * 2 + [pl.BlockSpec((TILE, width), lambda i, s: (i, 0))],
            out_specs=tuple(pl.BlockSpec((TILE, n), lambda i, s: (i, 0)) for n in (4 * width, width)),
        ),
        out_shape=(jax.ShapeDtypeStruct((rows, 4 * width), jnp.bfloat16), jax.ShapeDtypeStruct(q.shape, jnp.float32)),
        compiler_params=pltpu.CompilerParams(vmem_limit_bytes=LIMIT),
        cost_estimate=pl.CostEstimate(flops=100_000_000, bytes_accessed=25_000_000, transcendentals=0),
        name="split",
    )(source, a, b, ours, theirs, q)


def columns_kernel(factor, panel, ih, il, ah, al, g, q):
    g[...], q[...] = column_tile(factor[...], panel[...], ih, il, ah, al)


def columns(factor, panel, weights):
    rows, width = factor.shape
    spec = pl.BlockSpec((TILE, width), lambda i: (i, 0))
    fixed = pl.BlockSpec((width, width), lambda i: (0, 0))
    out = jax.ShapeDtypeStruct((rows, width), jnp.float32)
    return pl.pallas_call(
        columns_kernel,
        grid=(pl.cdiv(rows, TILE),),
        in_specs=[spec, spec] + [fixed] * 4,
        out_specs=(spec, spec),
        out_shape=(out, out),
        compiler_params=pltpu.CompilerParams(vmem_limit_bytes=LIMIT),
        cost_estimate=pl.CostEstimate(flops=18 * rows * width * width, bytes_accessed=16 * rows * width, transcendentals=0),
        name="columns",
    )(factor, panel, *weights)


def update_kernel(tiles, slab, g, q, trailing, *refs):
    out, full, half = refs[-3:]
    width = g.shape[1]

    @pl.when(pl.program_id(1) == 0)
    def _():
        gh, half[:, :width] = halves(g[...])
        qh, half[:, width:] = halves(q[...])
        full[:, :width] = gh
        full[:, width:2 * width] = gh
        full[:, 2 * width:3 * width] = qh
        full[:, 3 * width:] = qh

    u = dot(slab[...], full[...], True) + dot(slab[:, width:3 * width], half[...], True)
    out[...] = trailing[...] - u


def update(trailing, slab, g, q, tiles, out, offset=None, tile=TILE):
    rows, width = slab.shape[0], g.shape[1]
    step = 512
    count = tiles.shape[0]
    part = pl.BlockSpec((step, 4 * width), lambda i, j, t: (j, 0))
    tall = pl.BlockSpec((step, tile), lambda i, j, t: (j, t[i]))
    wide = pl.BlockSpec((tile, width), lambda i, j, t: (i, 0))
    if offset is not None:
        over = 2 * tile
        wide = pl.BlockSpec(
            (pl.Element(tile, padding=(0, over)), pl.Element(width)),
            lambda i, j, t: (pl.multiple_of(i * tile + t[count], 8), 0))
        tiles = jnp.concatenate([tiles, jnp.reshape(offset, (1,)).astype(jnp.int32)])
    args = [tiles, slab, g, q, trailing]
    specs = [part, wide, wide, tall]
    alias = {}
    if out is not None:
        alias = {len(args): 0}
        args.append(out)
        specs.append(ANY)
    return pl.pallas_call(
        update_kernel,
        grid_spec=pltpu.PrefetchScalarGridSpec(
            num_scalar_prefetch=1, grid=(count, pl.cdiv(rows, step)), in_specs=specs, out_specs=tall,
            scratch_shapes=[pltpu.VMEM((tile, 4 * width), jnp.bfloat16), pltpu.VMEM((tile, 2 * width), jnp.bfloat16)]),
        out_shape=jax.ShapeDtypeStruct(trailing.shape, jnp.float32),
        input_output_aliases=alias,
        compiler_params=pltpu.CompilerParams(vmem_limit_bytes=LIMIT),
        cost_estimate=pl.CostEstimate(flops=12 * rows * width * tile * count, bytes_accessed=12 * rows * tile * count, transcendentals=0),
        name="update",
    )(*args)


def make_fast(ncol, devices):
    swap = [(0, 1), (1, 0)]

    def body(trailing, panel_block, factor_panel, corner_block, corner_inverse):
        rows, _ = panel_block.shape
        d = lax.axis_index("depth")
        low = rows // TILE
        shift = (low + 1) * TILE - rows

        def send(value):
            return lax.ppermute(value, "depth", swap)

        early = low - 1
        first = early * TILE + shift
        packed = pack_corner(corner_block, corner_inverse)
        theirs = send(packed)
        pair = jnp.where(d == 1, jnp.concatenate([theirs, packed], axis=0), jnp.concatenate([packed, theirs], axis=0))
        factor_raw = send(factor_panel[:first])
        panel_raw = send(panel_block[:first])

        sent = (TILE, rows - first - TILE, shift, rows - low * TILE)
        ps, fs, *more = spread(pair, panel_block, factor_panel, corner_inverse.shape[0], sent, ncol, devices)
        weights, (g, q, corner_out) = more[:4], more[4:7]
        ends = more[7:11], more[11:]
        source = (lax.axis_index(("row", "col")) == 0).astype(jnp.int32)
        slab, panel_out = split(ps, fs, panel_block, factor_panel, q, jnp.reshape(source, (1,)))

        def ids(first, count):
            return (first + jnp.arange(count)).astype(jnp.int32)

        base = d * (low + 1)
        other = (1 - d) * (low + 1)
        size = 2 * TILE if (low + 1) % 2 == 0 and early % 2 == 0 else TILE
        second = []
        for v in ends:
            second.append(send(v[0]))

        out = update(trailing, slab, g, q, ids(base * TILE // size, pl.cdiv(rows - shift, size)), None, shift * d, size)
        third = [send(v) for v in after([v[1] for v in ends], out)]

        early_cols = columns(*after((factor_raw, panel_raw), out), weights)
        out = update(trailing, slab, *early_cols, ids(other * TILE // size, early * TILE // size), out, shift * (1 - d), size)

        def middle(have, came, mine):
            ahead = jnp.concatenate([have[early * TILE:], came[:TILE - shift]], axis=0)
            across = jnp.concatenate([mine[3], have[:shift]], axis=0)
            return jnp.concatenate([jnp.where(d == 1, ahead, came), jnp.where(d == 1, ahead, across)], axis=0)

        second = after(second, out)
        cols = [middle(*v) for v in zip(early_cols, second, ends)]
        out = update(trailing, slab, *cols, jnp.stack([other + early, jnp.where(d == 1, early, low)]).astype(jnp.int32), out)

        def final(came, end, mine):
            ahead = jnp.concatenate([came[TILE - shift:], end, mine[2]], axis=0)
            return jnp.where(d == 1, ahead, jnp.concatenate([end, came[:TILE - end.shape[0]]], axis=0))

        third = after(third, out)
        cols = [final(*v) for v in zip(second, third, ends)]
        out = update(trailing, slab, *cols, ids(other + low, 1), out)
        return (out, panel_out, corner_out)

    return body


def solution(mesh):
    in_specs = (
        P("depth", ("row", "col")),
        P(EVERY, None),
        P(EVERY, None),
        P(EVERY, None),
        P(EVERY, None),
    )
    out_specs = (
        P("depth", ("row", "col")),
        P(EVERY, None),
        P(EVERY, None),
    )
    layers, nrow, ncol = mesh.shape["depth"], mesh.shape["row"], mesh.shape["col"]
    general = make_general(layers)

    def body(*args):
        rows = args[1].shape[0]
        unit = args[4].shape[0]
        fits = layers == 2 and nrow == 4 and ncol > 1 and rows % 32 == 0 and rows > 4 * TILE and args[1].shape[1] % TILE == 0
        fits = fits and rows % TILE + unit == TILE and unit % 8 == 0
        chosen = make_fast(ncol, layers * nrow * ncol) if fits else general
        return chosen(*args)

    return jax.shard_map(body, mesh=mesh, in_specs=in_specs, out_specs=out_specs, check_vma=False)
```
